32 devices in a mesh: row: 4 (over z), col: 8 (over y, x, core).
Axes of the slice: x: 2, y: 2, z: 4, core: 2. Of those that a mesh axis runs over, the one named last changes fastest.
Arguments:
- matrix: float32 [15360, 15360], P('row', 'col'), may hold values from -4 to 4
- rhs: float32 [15360, 4096], P('row', 'col'), may hold values from -6 to 6
- pivot_inverses: bfloat16 [2, 512, 512], replicated, may hold values from -0.046875 to 0.046875
- panel_order: int32 [2], replicated, may hold values from 0 to 29, as said below
Outputs:
- factored: bfloat16 [15360, 15360], P('row', 'col')
- updated_rhs: float32 [15360, 4096], P('row', 'col')
- rhs_norms: float32 [4096], P('col')
The draws below stay inside these ranges and needn't reach their ends.
Inputs may be any that keep to these rules, and one draw needn't show every extreme that they name: `panel_order`: two different panel indices, one of which is the last panel, 29.
All inputs are finite; a program needn't handle non-finite values.
Results may differ from the reference program's by a relative error of at most 0.001.
Values sent between devices are 32-bit elements; how exact they have to be, the bound alone decides.
No kernel may reach another device: no remote copies, remote signals or barrier semaphores. Data moves between devices by JAX's collectives and lax.ppermute only.
A program may use at most 192 MiB of HBM per device.

```python
import jax
import jax.numpy as jnp
from jax import lax

N = 15360
PW = 512
NRHS = 4096
NB = 128
NP = 30
N_ROW = 4
N_COL = 8


def draw_panel_order(key, part):
    other = jax.random.randint(jax.random.fold_in(key, 7), (), 0, NP - 1).astype(jnp.int32)
    flip = jax.random.randint(jax.random.fold_in(key, 11), (), 0, 2).astype(jnp.int32)
    last = jnp.full((), NP - 1, jnp.int32)
    first_entry = jnp.where(flip == 0, other, last)
    second_entry = jnp.where(flip == 0, last, other)
    return jnp.stack([first_entry, second_entry]).astype(jnp.int32)


def level_of(key, dims, cuts, smallest, largest):
    level = 1.0
    for dim, shards_of in cuts:
        draws = jax.random.uniform(jax.random.fold_in(jax.random.fold_in(key, 6), dim), (shards_of,), jnp.float32, smallest / len(cuts), largest / len(cuts))
        level = level * jnp.repeat(jnp.exp(draws), dims[dim] // shards_of).reshape((-1,) + (1,) * (len(dims) - 1 - dim))
    return level


def noise(rng, extent, deviation, reach, pieces=(), kind=jnp.bfloat16):
    drawn = jax.random.normal(rng, extent, jnp.float32) * deviation
    if len(pieces) > 0:
        drawn = level_of(rng, extent, pieces, -0.22, 0.18) * drawn
    return jnp.clip(drawn, min=-reach, max=reach).astype(kind)


def setup_inputs(seed: int = 0) -> dict:
    key_list = jax.random.split(jax.random.key(seed), 5)
    matrix = noise(key_list[0], (N, N), 0.25, 4.0, ((0, 4), (1, 8)), jnp.float32)
    rhs = noise(key_list[1], (N, NRHS), 1.0, 6.0, ((0, 4), (1, 8)), jnp.float32)
    pivot_inverses = noise(key_list[2], (2, PW, PW), (32 * PW) ** -0.5, 0.046875)
    panel_order = draw_panel_order(jax.random.fold_in(key_list[4], 71), 0)
    return {"matrix": matrix, "rhs": rhs, "pivot_inverses": pivot_inverses, "panel_order": panel_order}


def stored_rows(global_ids):
    blocks = global_ids // NB
    return blocks % N_ROW * (N // N_ROW) + blocks // N_ROW * NB + global_ids % NB

def stored_cols(global_ids):
    blocks = global_ids // NB
    return blocks % N_COL * (N // N_COL) + blocks // N_COL * NB + global_ids % NB

def product(first, second):
    return jnp.dot(first, second, precision=lax.Precision.HIGHEST, preferred_element_type=jnp.float32)

def reference(matrix, rhs, pivot_inverses, panel_order):
    current = matrix
    right_sides = rhs
    keep_row = jnp.ones((N,), jnp.float32)
    keep_col = jnp.ones((N,), jnp.float32)
    for section in range(2):
        panel_id = panel_order[section]
        global_ids = (panel_id * PW + jnp.arange(PW, dtype=jnp.int32)).astype(jnp.int32)
        row_ids = stored_rows(global_ids).astype(jnp.int32)
        col_ids = stored_cols(global_ids).astype(jnp.int32)
        keep_row = keep_row.at[row_ids].set(0.0)
        keep_col = keep_col.at[col_ids].set(0.0)
        panel_cols = current[:, col_ids]
        upper_rows = current[row_ids, :]
        rhs_rows = right_sides[row_ids, :]
        multipliers = product(panel_cols, pivot_inverses[section].astype(jnp.float32))
        update = product(multipliers, upper_rows * keep_col[None, :])
        updated = current - keep_row[:, None] * update
        panel_values = jnp.where(keep_row[:, None] > 0, multipliers, panel_cols)
        current = updated.at[:, col_ids].set(panel_values)
        right_sides = right_sides - keep_row[:, None] * product(multipliers, rhs_rows)
    rhs_norms = jnp.sqrt(lax.optimization_barrier(jnp.sum(right_sides * right_sides, axis=0)) / N + 1e-06)
    return (current.astype(jnp.bfloat16), right_sides, rhs_norms)
```

```python
import functools

import jax
import jax.numpy as jnp
from jax import lax
from jax.experimental import pallas as pl
from jax.experimental.pallas import tpu as pltpu
from jax.sharding import PartitionSpec as P

LANES = 128
F32 = jnp.float32
BF16 = jnp.bfloat16


def split(values):
    high = values.astype(BF16)
    return high, (values - high.astype(F32)).astype(BF16)


def dot(first, second):
    return jnp.dot(first, second, preferred_element_type=F32)


def dot3(first, second):
    (fh, fl), (sh, sl) = first, second
    return dot(fh, sh) + dot(fh, sl) + dot(fl, sh)


def dot2(first, second):
    fh, fl = first
    return dot(fh, second) + dot(fl, second)


def factors_tile(ca, cb, row_block, a, b, inv_a, inv_b, w_ab, pivot_rows):
    in_a, in_b = row_block == a, row_block == b
    m_a = dot2(split(ca), inv_a)
    new_b = cb - dot3(split(m_a), w_ab)
    m_b = dot2(split(new_b), inv_b)
    left_a = m_a - dot3(split(m_b), pivot_rows)
    left_a = jnp.where(in_a, 0.0, jnp.where(in_b, m_a, left_a))
    left_b = jnp.where(in_a | in_b, 0.0, m_b)
    return m_a, new_b, m_b, left_a, left_b


def factors_kernel(
    n_blocks, block, first_row, n_kept, scalars, *refs
):
    ca_refs, cb_refs = refs[:n_blocks], refs[n_blocks : 2 * n_blocks]
    inv_a, inv_b, w_ab, w_ba = refs[2 * n_blocks : 2 * n_blocks + 4]
    out = refs[2 * n_blocks + 4 + n_kept :]
    high_ref, low_ref, fa_ref, fb_ref, wh, wl, ph, pll, ma_s, nb_s, mb_s = out
    a, b, own = scalars[0], scalars[1], scalars[2]

    @pl.when(pl.program_id(0) == 0)
    def _():
        wh[...], wl[...] = split(w_ab[...])
        ph[...], pll[...] = split(dot2(split(w_ba[...]), inv_a[...]))

    rows = high_ref.shape[0]
    start = first_row + pl.program_id(0) * rows
    row_block = (start + lax.broadcasted_iota(jnp.int32, (rows, 1), 0)) // block
    ca = jnp.concatenate([r[...] for r in ca_refs], axis=1)
    cb = jnp.concatenate([r[...] for r in cb_refs], axis=1)
    m_a, new_b, m_b, left_a, left_b = factors_tile(
        ca, cb, row_block, a, b, inv_a[...], inv_b[...],
        (wh[...], wl[...]), (ph[...], pll[...]),
    )
    for left, shift in ((left_a, 0), (left_b, 1)):
        high, low = split(left)
        for r in range(n_blocks):
            there = pl.ds((2 * r + shift) * block, block)
            high_ref[:, there] = high[:, r * block : (r + 1) * block]
            low_ref[:, there] = low[:, r * block : (r + 1) * block]
    ma_s[...], mb_s[...] = m_a, m_b
    mine = pl.ds(pl.multiple_of(own * block, block), block)
    in_a, in_b = row_block == a, row_block == b
    fa_ref[...] = jnp.where(in_a, ca_refs[0][...], ma_s[:, mine]).astype(BF16)
    fb_ref[...] = jnp.where(
        in_a, cb_refs[0][...], jnp.where(in_b, new_b[:, :block], mb_s[:, mine])
    ).astype(BF16)


def factors(ca, cb, inv_a, inv_b, w_ab, w_ba, scalars, row_len, first_row, kept):
    n_blocks, (rows, block) = len(ca), ca[0].shape
    width = n_blocks * block
    tile = tile_of(rows, 384, block)
    first = first_row // tile
    slab = pl.BlockSpec((tile, block), lambda i, s: (i, 0))
    whole = pl.BlockSpec((width, width), lambda i, s: (0, 0))
    shapes = (
        jax.ShapeDtypeStruct((row_len, 2 * width), BF16),
        jax.ShapeDtypeStruct((row_len, 2 * width), BF16),
        jax.ShapeDtypeStruct((row_len, block), BF16),
        jax.ShapeDtypeStruct((row_len, block), BF16),
    )
    n_in = 1 + 2 * n_blocks + 4
    return pl.pallas_call(
        functools.partial(factors_kernel, n_blocks, block, first_row, len(kept)),
        grid_spec=pltpu.PrefetchScalarGridSpec(
            num_scalar_prefetch=1,
            grid=(rows // tile,),
            in_specs=[slab] * (2 * n_blocks)
            + [whole] * 4
            + [pl.BlockSpec(memory_space=pl.ANY)] * len(kept),
            out_specs=[
                pl.BlockSpec((tile, s.shape[1]), lambda i, s: (first + i, 0))
                for s in shapes
            ],
            scratch_shapes=[pltpu.VMEM((width, width), BF16)] * 4
            + [pltpu.VMEM((tile, width), F32)] * 3,
        ),
        out_shape=shapes,
        input_output_aliases={n_in + i: i for i in range(len(kept))},
        name="factors",
    )(scalars, *ca, *cb, inv_a, inv_b, w_ab, w_ba, *kept)


def tile_of(size, most, unit):
    for count in range(1, size // unit + 1):
        if size % (count * unit) == 0 and size // count <= most:
            return size // count
    return unit


def matrix_kernel(block, first_tile, n_kept, scalars, a_ref, high, low, upper, fa, fb, *refs):
    out_ref, uh, ul = refs[n_kept:]

    @pl.when(pl.program_id(1) == 0)
    def _():
        uh[...], ul[...] = split(upper[...])

    update = dot3((high[...], low[...]), (uh[...], ul[...]))
    out_ref[...] = (a_ref[...] - update).astype(BF16)
    width = out_ref.shape[1]
    left_edge = (first_tile + pl.program_id(0)) * width
    for slot, final in ((0, fa), (1, fb)):
        offset = scalars[3 + slot] - left_edge

        @pl.when((scalars[5 + slot] > 0) & (offset >= 0) & (offset < width))
        def _(final=final, offset=offset):
            out_ref[:, pl.ds(pl.multiple_of(offset, block), block)] = final[...]


def update_matrix(matrix, high, low, upper, fa, fb, scalars, first_col, block, tn, kept):
    rows, cols = matrix.shape
    depth, width = upper.shape
    tm = tile_of(rows, 384, block)
    first = first_col // tn
    here = pl.BlockSpec((tm, tn), lambda j, i, s: (i, first + j))
    left = pl.BlockSpec((tm, depth), lambda j, i, s: (i, 0))
    final = pl.BlockSpec((tm, block), lambda j, i, s: (i, 0))
    return pl.pallas_call(
        functools.partial(matrix_kernel, block, first, len(kept)),
        grid_spec=pltpu.PrefetchScalarGridSpec(
            num_scalar_prefetch=1,
            grid=(width // tn, rows // tm),
            in_specs=[
                here, left, left,
                pl.BlockSpec((depth, tn), lambda j, i, s: (0, j)),
                final, final,
            ]
            + [pl.BlockSpec(memory_space=pl.ANY)] * len(kept),
            out_specs=here,
            scratch_shapes=[pltpu.VMEM((depth, tn), BF16)] * 2,
        ),
        out_shape=jax.ShapeDtypeStruct((rows, cols), BF16),
        input_output_aliases={7: 0} if kept else {},
        name="update_matrix",
    )(scalars, matrix, high, low, upper, fa, fb, *kept)


def rhs_kernel(r_ref, high, low, upper, out_ref, sums_ref, uh, ul):
    @pl.when(pl.program_id(0) == 0)
    def _():
        uh[...], ul[...] = split(upper[...])
        sums_ref[...] = jnp.zeros_like(sums_ref)

    new = r_ref[...] - dot3((high[...], low[...]), (uh[...], ul[...]))
    out_ref[...] = new
    sums_ref[...] += jnp.sum(new * new, axis=0, keepdims=True)


def update_rhs(rhs, high, low, upper, block):
    rows, cols = rhs.shape
    depth = upper.shape[0]
    tm = tile_of(rows, 384, block)
    here = pl.BlockSpec((tm, cols), lambda i: (i, 0))
    left = pl.BlockSpec((tm, depth), lambda i: (i, 0))
    return pl.pallas_call(
        rhs_kernel,
        grid=(rows // tm,),
        in_specs=[here, left, left, pl.BlockSpec((depth, cols), lambda i: (0, 0))],
        out_specs=[here, pl.BlockSpec((1, cols), lambda i: (0, 0))],
        out_shape=[
            jax.ShapeDtypeStruct(rhs.shape, F32),
            jax.ShapeDtypeStruct((1, cols), F32),
        ],
        scratch_shapes=[pltpu.VMEM((depth, cols), BF16)] * 2,
        name="update_rhs",
    )(rhs, high, low, upper)


def on_device(matrix, rhs, pivot_inverses, panel_order):
    row_count, col_count = lax.axis_size("row"), lax.axis_size("col")
    width = pivot_inverses.shape[1]
    block = width // row_count
    groups = col_count // row_count
    row_len, col_len = matrix.shape
    total_rows = row_len * row_count
    rhs_len = rhs.shape[1]
    col_index = lax.axis_index("col")
    own, group = col_index % row_count, col_index // row_count
    a, b = panel_order[0], panel_order[1]
    owns = [group == p % groups for p in (a, b)]
    offsets = [p // groups * block for p in (a, b)]
    masks = [0]
    bits = [row_count >> (k + 1) for k in range(row_count.bit_length() - 1)]
    for bit in bits:
        masks = masks + [m ^ bit for m in masks]

    def from_owner(piece, panel):
        chosen = piece
        for step in range(1, groups):
            moved = lax.ppermute(
                piece, "col",
                [(i, (i + step * row_count) % col_count) for i in range(col_count)],
            )
            chosen = jnp.where((group - step) % groups == panel % groups, moved, chosen)
        return chosen

    def spread(piece):
        pieces = [piece]
        for bit in bits:
            swap = [(i, i ^ bit) for i in range(col_count)]
            pieces = pieces + [lax.ppermute(p, "col", swap) for p in pieces]
        return pieces

    panel_rows = [lax.dynamic_slice_in_dim(matrix, p * block, block, 0) for p in (a, b)]
    rhs_rows = [lax.dynamic_slice_in_dim(rhs, p * block, block, 0) for p in (a, b)]
    cross = [
        lax.dynamic_slice_in_dim(panel_rows[0], offsets[1], block, 1),
        lax.dynamic_slice_in_dim(panel_rows[1], offsets[0], block, 1),
    ]
    gather = functools.partial(lax.all_gather, axis_name="row", axis=0, tiled=True)
    head = gather(
        jnp.concatenate(
            [jnp.concatenate([r, c], axis=1) for r, c in zip(rhs_rows, cross)], axis=0
        )
    )
    aligned = block % LANES == 0 and col_len % LANES == 0 and rhs_len % LANES == 0
    tn = tile_of(col_len, 640, block) if aligned else col_len
    n_tiles = col_len // tn
    cut = (n_tiles + 1) // 2 * tn
    both = jnp.concatenate(panel_rows, axis=0)
    uppers = [gather(both[:, :cut])]
    if cut < col_len:
        uppers.append(gather(both[:, cut:]))
    rhs_upper, crossing = head[:, :rhs_len], head[:, rhs_len:]

    halves = 2 if row_len % (2 * block) == 0 else 1
    part = row_len // halves
    slabs = []
    for h in range(halves):
        for p, offset in zip((a, b), offsets):
            piece = lax.dynamic_slice(matrix, (h * part, offset), (part, block))
            slabs.append(spread(from_owner(piece, p)))
    crossing = crossing.reshape(row_count, 2, block, block)
    w_ab = from_owner(crossing[:, 0].reshape(width, block), b)
    w_ba = from_owner(crossing[:, 1].reshape(width, block), a)
    pieces = spread(jnp.concatenate([w_ab, w_ba], axis=0))
    w_ab = jnp.concatenate([p[:width] for p in pieces], axis=1)
    w_ba = jnp.concatenate([p[width:] for p in pieces], axis=1)
    inverses = [
        jnp.concatenate(
            [
                lax.dynamic_slice_in_dim(pivot_inverses[s], (own ^ m) * block, block, 0)
                for m in masks
            ],
            axis=0,
        )
        for s in range(2)
    ]

    if aligned:
        scalars = jnp.stack(
            [a, b, own, offsets[0], offsets[1]] + [o.astype(jnp.int32) for o in owns]
        ).astype(jnp.int32)
        kept = ()
        for h in range(halves):
            kept = factors(
                slabs[2 * h], slabs[2 * h + 1], *inverses, w_ab, w_ba,
                scalars, row_len, h * part, kept,
            )
        high, low, fa, fb = kept
        new_rhs, sums = update_rhs(rhs, high, low, rhs_upper, block)
        out = ()
        for k, upper in enumerate(uppers):
            out = (
                update_matrix(
                    matrix, high, low, upper, fa, fb, scalars, k * cut, block, tn, out
                ),
            )
        factored, sums = out[0], sums[0]
    else:
        row_block = (jnp.arange(row_len, dtype=jnp.int32) // block)[:, None]
        ca, cb = [
            jnp.concatenate(
                [jnp.concatenate(slabs[2 * h + s], axis=1) for h in range(halves)], axis=0
            )
            for s in range(2)
        ]
        m_a, new_b, m_b, left_a, left_b = factors_tile(
            ca, cb, row_block, a, b, *inverses, split(w_ab),
            split(dot2(split(w_ba), inverses[0])),
        )
        left = split(
            jnp.stack(
                [x.reshape(row_len, row_count, block) for x in (left_a, left_b)], axis=2
            ).reshape(row_len, 2 * width)
        )
        new_rhs = rhs - dot3(left, split(rhs_upper))
        sums = jnp.sum(new_rhs * new_rhs, axis=0)
        current = matrix - dot3(left, split(jnp.concatenate(uppers, axis=1)))
        in_a, in_b = row_block == a, row_block == b
        mine = [
            lax.dynamic_slice_in_dim(m, own * block, block, 1) for m in (m_a, m_b)
        ]
        final = (
            jnp.where(in_a, ca[:, :block], mine[0]),
            jnp.where(in_a, cb[:, :block], jnp.where(in_b, new_b[:, :block], mine[1])),
        )
        for values, offset, is_owner in zip(final, offsets, owns):
            old = lax.dynamic_slice_in_dim(current, offset, block, 1)
            current = lax.dynamic_update_slice_in_dim(
                current, jnp.where(is_owner, values, old), offset, 1
            )
        factored = current.astype(BF16)
    totals = lax.psum(sums, "row")
    rhs_norms = jnp.sqrt(totals / total_rows + 1e-06)
    return factored, new_rhs, rhs_norms


def solution(mesh):
    in_specs = (P("row", "col"), P("row", "col"), P(), P())
    out_specs = (P("row", "col"), P("row", "col"), P("col"))
    return jax.shard_map(
        on_device, mesh=mesh, in_specs=in_specs, out_specs=out_specs, check_vma=False
    )
```

```python
import functools

import jax
import jax.numpy as jnp
from jax import lax
from jax.experimental import pallas as pl
from jax.experimental.pallas import tpu as pltpu
from jax.sharding import PartitionSpec as P

LANES = 128
F32 = jnp.float32
BF16 = jnp.bfloat16
F8 = jnp.float8_e4m3fn
ROW_TOP, LOW_UP, UPPER_UP, UPPER_LOW_UP = 224.0, 2.0**8, 2.0**6, 2.0**14


def cost_of(products, size):
    return pl.CostEstimate(flops=2 * products, bytes_accessed=size, transcendentals=0)


def split(values):
    high = values.astype(BF16)
    return high, (values - high.astype(F32)).astype(BF16)


def dot(first, second):
    return jnp.dot(first, second, preferred_element_type=F32)


def dot3(first, second):
    (fh, fl), (sh, sl) = first, second
    return dot(fh, sh) + dot(fh, sl) + dot(fl, sh)


def dot2(first, second):
    fh, fl = first
    return dot(fh, second) + dot(fl, second)


def factors_tile(ca, cb, row_block, a, b, inv_a, inv_b, w_ab, pivot_rows):
    in_a, in_b = row_block == a, row_block == b
    m_a = dot2(split(ca), inv_a)
    new_b = cb - dot3(split(m_a), w_ab)
    m_b = dot2(split(new_b), inv_b)
    left_a = m_a - dot3(split(m_b), pivot_rows)
    left_a = jnp.where(in_a, 0.0, jnp.where(in_b, m_a, left_a))
    left_b = jnp.where(in_a | in_b, 0.0, m_b)
    return m_a, new_b, m_b, left_a, left_b


def factors_kernel(
    n_blocks, block, first_row, n_kept, scalars, *refs
):
    rhs_ref, upper_ref, *refs = refs
    ca_refs, cb_refs = refs[:n_blocks], refs[n_blocks : 2 * n_blocks]
    inv_a, inv_b, w_ab, w_ba = refs[2 * n_blocks : 2 * n_blocks + 4]
    out = refs[2 * n_blocks + 4 + n_kept :]
    high_ref, small_ref, scale_ref, fa_ref, fb_ref, new_rhs_ref, sums_ref, *scratch = out
    wh, wl, ph, pll, ma_s, mb_s, uh, ul, low_ref = scratch
    a, b, own = scalars[0], scalars[1], scalars[2]

    @pl.when(pl.program_id(0) == 0)
    def _():
        wh[...], wl[...] = split(w_ab[...])
        ph[...], pll[...] = split(dot2(split(w_ba[...]), inv_a[...]))
        uh[...], ul[...] = split(upper_ref[...])
        sums_ref[...] = jnp.zeros_like(sums_ref)

    rows = high_ref.shape[0]
    start = first_row + pl.program_id(0) * rows
    row_block = (start + lax.broadcasted_iota(jnp.int32, (rows, 1), 0)) // block
    ca = jnp.concatenate([r[...] for r in ca_refs], axis=1)
    cb = jnp.concatenate([r[...] for r in cb_refs], axis=1)
    m_a, new_b, m_b, left_a, left_b = factors_tile(
        ca, cb, row_block, a, b, inv_a[...], inv_b[...],
        (wh[...], wl[...]), (ph[...], pll[...]),
    )
    top = jnp.maximum(
        jnp.max(jnp.maximum(jnp.abs(left_a), jnp.abs(left_b)), axis=1, keepdims=True),
        1e-30,
    )
    up = ROW_TOP / top
    scale_ref[...] = top / (ROW_TOP * UPPER_LOW_UP)
    depth = high_ref.shape[1]
    for left, shift in ((left_a, 0), (left_b, 1)):
        high = left.astype(BF16)
        rest = left - high.astype(F32)
        low = rest.astype(BF16)
        small_high = (left * up).astype(F8)
        small_low = (rest * (up * LOW_UP)).astype(F8)
        for r in range(n_blocks):
            start, here = (2 * r + shift) * block, slice(r * block, (r + 1) * block)
            high_ref[:, pl.ds(start, block)] = high[:, here]
            low_ref[:, pl.ds(start, block)] = low[:, here]
            small_ref[:, pl.ds(start, block)] = small_high[:, here]
            small_ref[:, pl.ds(depth + start, block)] = small_low[:, here]
    ma_s[...], mb_s[...] = m_a, m_b
    mine = pl.ds(pl.multiple_of(own * block, block), block)
    in_a, in_b = row_block == a, row_block == b
    fa_ref[...] = jnp.where(in_a, ca_refs[0][...], ma_s[:, mine]).astype(BF16)
    fb_ref[...] = jnp.where(
        in_a, cb_refs[0][...], jnp.where(in_b, new_b[:, :block], mb_s[:, mine])
    ).astype(BF16)
    new_rhs = rhs_ref[...] - dot3((high_ref[...], low_ref[...]), (uh[...], ul[...]))
    new_rhs_ref[...] = new_rhs
    sums_ref[...] += jnp.sum(new_rhs * new_rhs, axis=0, keepdims=True)


def factors(
    rhs, rhs_upper, ca, cb, inv_a, inv_b, w_ab, w_ba, scalars, first_row, kept
):
    row_len, rhs_len = rhs.shape
    n_blocks, (rows, block) = len(ca), ca[0].shape
    width = n_blocks * block
    tile = tile_of(rows, 640, 16)
    first = first_row // tile
    slab = pl.BlockSpec((tile, block), lambda i, s: (i, 0))
    whole = pl.BlockSpec((width, width), lambda i, s: (0, 0))

    def out_rows(columns):
        return pl.BlockSpec((tile, columns), lambda i, s: (first + i, 0))

    shapes = (
        jax.ShapeDtypeStruct((row_len, 2 * width), BF16),
        jax.ShapeDtypeStruct((row_len, 4 * width), F8),
        jax.ShapeDtypeStruct((row_len, 1), F32),
        jax.ShapeDtypeStruct((row_len, block), BF16),
        jax.ShapeDtypeStruct((row_len, block), BF16),
        jax.ShapeDtypeStruct(rhs.shape, F32),
        jax.ShapeDtypeStruct((1, rhs_len), F32),
    )
    n_in = 3 + 2 * n_blocks + 4
    *kept_out, sums = pl.pallas_call(
        functools.partial(factors_kernel, n_blocks, block, first_row, len(kept)),
        grid_spec=pltpu.PrefetchScalarGridSpec(
            num_scalar_prefetch=1,
            grid=(rows // tile,),
            in_specs=[
                out_rows(rhs_len),
                pl.BlockSpec((2 * width, rhs_len), lambda i, s: (0, 0)),
            ]
            + [slab] * (2 * n_blocks)
            + [whole] * 4
            + [pl.BlockSpec(memory_space=pl.ANY)] * len(kept),
            out_specs=[out_rows(s.shape[1]) for s in shapes[:-1]]
            + [pl.BlockSpec((1, rhs_len), lambda i, s: (0, 0))],
            scratch_shapes=[pltpu.VMEM((width, width), BF16)] * 4
            + [pltpu.VMEM((tile, width), F32)] * 2
            + [pltpu.VMEM((2 * width, rhs_len), BF16)] * 2
            + [pltpu.VMEM((tile, 2 * width), BF16)],
        ),
        out_shape=shapes,
        input_output_aliases={n_in + i: i for i in range(len(kept))},
        cost_estimate=cost_of(rows * (10 * width * width + 6 * width * rhs_len), rows * 8192),
        name="factors",
    )(scalars, rhs, rhs_upper, *ca, *cb, inv_a, inv_b, w_ab, w_ba, *kept)
    return kept_out, sums


def column_cuts(size):
    units = size // LANES
    if size % LANES or units < 6:
        return [0, size]
    return [0, units * 3 // 4 * LANES, size]


def tile_of(size, most, unit):
    for count in range(1, size // unit + 1):
        if size % (count * unit) == 0 and size // count <= most:
            return size // count
    return unit


def matrix_kernel(block, first_col, n_kept, scalars, a_ref, high, small, scale, upper, fa, fb, *refs):
    out_ref, uh, us = refs[n_kept:]

    @pl.when(pl.program_id(0) == 0)
    def _():
        depth = upper.shape[0]
        top = upper[...].astype(BF16)
        uh[...] = top
        us[:depth] = ((upper[...] - top.astype(F32)) * UPPER_LOW_UP).astype(F8)
        us[depth:] = (upper[...] * UPPER_UP).astype(F8)

    update = dot(high[...], uh[...]) + dot(small[...], us[...]) * scale[...]
    out_ref[...] = (a_ref[...] - update).astype(BF16)
    width = out_ref.shape[1]
    for slot, final in ((0, fa), (1, fb)):
        offset = scalars[3 + slot] - first_col

        @pl.when((scalars[5 + slot] > 0) & (offset >= 0) & (offset < width))
        def _(final=final, offset=offset):
            out_ref[:, pl.ds(pl.multiple_of(offset, block), block)] = final[...]


def update_matrix(matrix, high, small, scale, upper, fa, fb, scalars, first_col, block, kept):
    rows, cols = matrix.shape
    depth, width = upper.shape
    tm = tile_of(rows, 768, block)
    here = pl.BlockSpec(
        (pl.Element(tm), pl.Element(width)), lambda i, s: (i * tm, first_col)
    )
    left = pl.BlockSpec((tm, depth), lambda i, s: (i, 0))
    final = pl.BlockSpec((tm, block), lambda i, s: (i, 0))
    return pl.pallas_call(
        functools.partial(matrix_kernel, block, first_col, len(kept)),
        grid_spec=pltpu.PrefetchScalarGridSpec(
            num_scalar_prefetch=1,
            grid=(rows // tm,),
            in_specs=[
                here, left,
                pl.BlockSpec((tm, 2 * depth), lambda i, s: (i, 0)),
                pl.BlockSpec((tm, 1), lambda i, s: (i, 0)),
                pl.BlockSpec((depth, width), lambda i, s: (0, 0)),
                final, final,
            ]
            + [pl.BlockSpec(memory_space=pl.ANY)] * len(kept),
            out_specs=here,
            scratch_shapes=[
                pltpu.VMEM((depth, width), BF16), pltpu.VMEM((2 * depth, width), F8)
            ],
        ),
        out_shape=jax.ShapeDtypeStruct((rows, cols), BF16),
        input_output_aliases={8: 0} if kept else {},
        cost_estimate=cost_of(3 * rows * depth * width, rows * width * 8),
        name="update_matrix",
    )(scalars, matrix, high, small, scale, upper, fa, fb, *kept)


def on_device(matrix, rhs, pivot_inverses, panel_order):
    row_count, col_count = lax.axis_size("row"), lax.axis_size("col")
    width = pivot_inverses.shape[1]
    block = width // row_count
    groups = col_count // row_count
    row_len, col_len = matrix.shape
    total_rows = row_len * row_count
    rhs_len = rhs.shape[1]
    col_index = lax.axis_index("col")
    own, group = col_index % row_count, col_index // row_count
    a, b = panel_order[0], panel_order[1]
    owns = [group == p % groups for p in (a, b)]
    offsets = [p // groups * block for p in (a, b)]
    masks = [0]
    bits = [row_count >> (k + 1) for k in range(row_count.bit_length() - 1)]
    for bit in bits:
        masks = masks + [m ^ bit for m in masks]

    def after(piece, event):
        return lax.optimization_barrier((piece, event))[0]

    def from_owner(piece, panel, event=None):
        chosen = piece
        for step in range(1, groups):
            moved = lax.ppermute(
                piece, "col",
                [(i, (i + step * row_count) % col_count) for i in range(col_count)],
            )
            if event is not None:
                moved = after(moved, event)
            chosen = jnp.where((group - step) % groups == panel % groups, moved, chosen)
        return chosen

    def spread(pieces, bits):
        for bit in bits:
            swap = [(i, i ^ bit) for i in range(col_count)]
            pieces = pieces + [lax.ppermute(p, "col", swap) for p in pieces]
        return pieces

    parts = 3 if row_len % (3 * 32) == 0 else 1
    part = row_len // parts
    pieces = [
        lax.dynamic_slice(matrix, (h * part, offset), (part, block))
        for h in range(parts)
        for offset in offsets
    ]

    def rows_of(array):
        return [lax.dynamic_slice_in_dim(array, p * block, block, 0) for p in (a, b)]

    cross = [
        lax.dynamic_slice(matrix, (a * block, offsets[1]), (block, block)),
        lax.dynamic_slice(matrix, (b * block, offsets[0]), (block, block)),
    ]
    rhs_rows, cross = after((rows_of(rhs), cross), pieces[:2])
    gather = functools.partial(lax.all_gather, axis_name="row", axis=0, tiled=True)
    head = gather(
        jnp.concatenate(
            [jnp.concatenate([c, r], axis=1) for r, c in zip(rhs_rows, cross)], axis=0
        )
    )
    aligned = block % LANES == 0 and col_len % LANES == 0 and rhs_len % LANES == 0
    cuts = column_cuts(col_len)
    panel_rows = after(rows_of(matrix), (rhs_rows, cross))
    strips = [
        jnp.concatenate([r[:, lo:hi] for r in panel_rows], axis=0)
        for lo, hi in zip(cuts, cuts[1:])
    ]
    uppers = [gather(strip) for strip in strips]

    chosen = [from_owner(p, (a, b)[n % 2]) for n, p in enumerate(pieces[:3])]
    far, last = bits[:-1], bits[-1:]
    slabs = [spread([piece], far) for piece in chosen[:2]]
    head = after(head, [slab[-1] for slab in slabs])
    crossing, rhs_upper = head[:, :block], head[:, block:]
    crossed = crossing.reshape(row_count, 2, block, block)
    w_ab = from_owner(crossed[:, 0].reshape(width, block), b)
    w_ba = from_owner(crossed[:, 1].reshape(width, block), a)
    pieces[3:4] = after(pieces[3:4], crossing)
    pieces[4:] = after(pieces[4:], (w_ab, w_ba))
    chosen += [from_owner(p, b) for p in pieces[3:4]]
    chosen[3:] = after(chosen[3:], (w_ab, w_ba))
    w_ab, w_ba = spread([w_ab], far), spread([w_ba], far)
    slabs += [spread([piece], far) for piece in chosen[2:]]
    w_ab, w_ba = [jnp.concatenate(spread(w, last), axis=1) for w in (w_ab, w_ba)]

    inverses = [
        jnp.concatenate(
            [
                lax.dynamic_slice_in_dim(pivot_inverses[s], (own ^ m) * block, block, 0)
                for m in masks
            ],
            axis=0,
        )
        for s in range(2)
    ]

    if aligned:
        scalars = jnp.stack(
            [a, b, own, offsets[0], offsets[1]] + [o.astype(jnp.int32) for o in owns]
        ).astype(jnp.int32)
        kept, all_sums = (), []
        for h in range(parts):
            pair = slabs[2 * h : 2 * h + 2]
            if h:
                pair = after(pair, all_sums[h - 1])
            kept, sums = factors(
                rhs, rhs_upper, *[spread(slab, last) for slab in pair], *inverses,
                w_ab, w_ba, scalars, h * part, kept,
            )
            all_sums.append(sums)
            if not h:
                slabs += [
                    spread([from_owner(p, (a, b)[n % 2], sums)], far)
                    for n, p in enumerate(pieces[4:])
                ]
        high, small, scale, fa, fb, new_rhs = kept
        out = ()
        for first_col, upper in zip(cuts, uppers):
            out = (
                update_matrix(
                    matrix, high, small, scale, upper, fa, fb, scalars, first_col, block, out
                ),
            )
        factored, sums = out[0], functools.reduce(jnp.add, all_sums)[0]
    else:
        slabs += [
            spread([from_owner(p, (a, b)[n % 2])], far) for n, p in enumerate(pieces[4:])
        ]
        slabs = [spread(slab, last) for slab in slabs]
        row_block = (jnp.arange(row_len, dtype=jnp.int32) // block)[:, None]
        ca, cb = [
            jnp.concatenate(
                [jnp.concatenate(slabs[2 * h + s], axis=1) for h in range(parts)], axis=0
            )
            for s in range(2)
        ]
        m_a, new_b, m_b, left_a, left_b = factors_tile(
            ca, cb, row_block, a, b, *inverses, split(w_ab),
            split(dot2(split(w_ba), inverses[0])),
        )
        left = split(
            jnp.stack(
                [x.reshape(row_len, row_count, block) for x in (left_a, left_b)], axis=2
            ).reshape(row_len, 2 * width)
        )
        new_rhs = rhs - dot3(left, split(rhs_upper))
        sums = jnp.sum(new_rhs * new_rhs, axis=0)
        current = matrix - dot3(left, split(jnp.concatenate(uppers, axis=1)))
        in_a, in_b = row_block == a, row_block == b
        mine = [
            lax.dynamic_slice_in_dim(m, own * block, block, 1) for m in (m_a, m_b)
        ]
        final = (
            jnp.where(in_a, ca[:, :block], mine[0]),
            jnp.where(in_a, cb[:, :block], jnp.where(in_b, new_b[:, :block], mine[1])),
        )
        for values, offset, is_owner in zip(final, offsets, owns):
            old = lax.dynamic_slice_in_dim(current, offset, block, 1)
            current = lax.dynamic_update_slice_in_dim(
                current, jnp.where(is_owner, values, old), offset, 1
            )
        factored = current.astype(BF16)
    totals = sums
    for bit in [1 << k for k in range(row_count.bit_length() - 1)]:
        totals = totals + lax.ppermute(
            totals, "row", [(i, i ^ bit) for i in range(row_count)]
        )
    rhs_norms = jnp.sqrt(totals / total_rows + 1e-06)
    return factored, new_rhs, rhs_norms


def solution(mesh):
    in_specs = (P("row", "col"), P("row", "col"), P(), P())
    out_specs = (P("row", "col"), P("row", "col"), P("col"))
    return jax.shard_map(
        on_device, mesh=mesh, in_specs=in_specs, out_specs=out_specs, check_vma=False
    )
```

```python
import functools

import jax
import jax.numpy as jnp
from jax import lax
from jax.experimental import pallas as pl
from jax.experimental.pallas import tpu as pltpu
from jax.sharding import PartitionSpec as P

LANES = 128
F32 = jnp.float32
BF16 = jnp.bfloat16
F8 = jnp.float8_e4m3fn
ROW_TOP, LOW_UP, UPPER_UP, UPPER_LOW_UP = 224.0, 2.0**8, 2.0**6, 2.0**14


def cost_of(products, size):
    return pl.CostEstimate(flops=2 * products, bytes_accessed=size, transcendentals=0)


def split(values):
    high = values.astype(BF16)
    return high, (values - high.astype(F32)).astype(BF16)


def dot(first, second):
    return jnp.dot(first, second, preferred_element_type=F32)


def dot3(first, second):
    (fh, fl), (sh, sl) = first, second
    return dot(fh, sh) + dot(fh, sl) + dot(fl, sh)


def dot2(first, second):
    fh, fl = first
    return dot(fh, second) + dot(fl, second)


def factors_tile(ca, cb, row_block, a, b, inv_a, inv_b, w_ab, pivot_rows):
    in_a, in_b = row_block == a, row_block == b
    m_a = dot2(split(ca), inv_a)
    new_b = cb - dot3(split(m_a), w_ab)
    m_b = dot2(split(new_b), inv_b)
    left_a = m_a - dot3(split(m_b), pivot_rows)
    left_a = jnp.where(in_a, 0.0, jnp.where(in_b, m_a, left_a))
    left_b = jnp.where(in_a | in_b, 0.0, m_b)
    return m_a, new_b, m_b, left_a, left_b


def prepare(upper, high, small):
    depth = upper.shape[0]
    top = upper[...].astype(BF16)
    high[...] = top
    small[:depth] = ((upper[...] - top.astype(F32)) * UPPER_LOW_UP).astype(F8)
    small[depth:] = (upper[...] * UPPER_UP).astype(F8)


def factors_kernel(
    n_blocks, block, first_row, n_kept, scalars, *refs
):
    rhs_ref, upper_ref, *refs = refs
    ca_refs, cb_refs = refs[:n_blocks], refs[n_blocks : 2 * n_blocks]
    inv_a, inv_b, w_ab, w_ba = refs[2 * n_blocks : 2 * n_blocks + 4]
    out = refs[2 * n_blocks + 4 + n_kept :]
    high_ref, small_ref, scale_ref, fa_ref, fb_ref, new_rhs_ref, sums_ref, *scratch = out
    wh, wl, ph, pll, ma_s, mb_s, uh, us = scratch
    a, b, own = scalars[0], scalars[1], scalars[2]

    @pl.when(pl.program_id(0) == 0)
    def _():
        wh[...], wl[...] = split(w_ab[...])
        ph[...], pll[...] = split(dot2(split(w_ba[...]), inv_a[...]))
        prepare(upper_ref, uh, us)
        sums_ref[...] = jnp.zeros_like(sums_ref)

    rows = high_ref.shape[0]
    start = first_row + pl.program_id(0) * rows
    row_block = (start + lax.broadcasted_iota(jnp.int32, (rows, 1), 0)) // block
    ca = jnp.concatenate([r[...] for r in ca_refs], axis=1)
    cb = jnp.concatenate([r[...] for r in cb_refs], axis=1)
    m_a, new_b, m_b, left_a, left_b = factors_tile(
        ca, cb, row_block, a, b, inv_a[...], inv_b[...],
        (wh[...], wl[...]), (ph[...], pll[...]),
    )
    top = jnp.maximum(
        jnp.max(jnp.maximum(jnp.abs(left_a), jnp.abs(left_b)), axis=1, keepdims=True),
        1e-30,
    )
    up = ROW_TOP / top
    scale_ref[...] = top / (ROW_TOP * UPPER_LOW_UP)
    depth = high_ref.shape[1]
    for left, shift in ((left_a, 0), (left_b, 1)):
        high = left.astype(BF16)
        rest = left - high.astype(F32)
        small_high = (left * up).astype(F8)
        small_low = (rest * (up * LOW_UP)).astype(F8)
        for r in range(n_blocks):
            start, here = (2 * r + shift) * block, slice(r * block, (r + 1) * block)
            high_ref[:, pl.ds(start, block)] = high[:, here]
            small_ref[:, pl.ds(start, block)] = small_high[:, here]
            small_ref[:, pl.ds(depth + start, block)] = small_low[:, here]
    ma_s[...], mb_s[...] = m_a, m_b
    mine = pl.ds(pl.multiple_of(own * block, block), block)
    in_a, in_b = row_block == a, row_block == b
    fa_ref[...] = jnp.where(in_a, ca_refs[0][...], ma_s[:, mine]).astype(BF16)
    fb_ref[...] = jnp.where(
        in_a, cb_refs[0][...], jnp.where(in_b, new_b[:, :block], mb_s[:, mine])
    ).astype(BF16)
    small = dot(small_ref[...], us[...]) * scale_ref[...]
    new_rhs = rhs_ref[...] - (dot(high_ref[...], uh[...]) + small)
    new_rhs_ref[...] = new_rhs
    sums_ref[...] += jnp.sum(new_rhs * new_rhs, axis=0, keepdims=True)


def factors(
    rhs, rhs_upper, ca, cb, inv_a, inv_b, w_ab, w_ba, scalars, first_row, kept
):
    row_len, rhs_len = rhs.shape
    n_blocks, (rows, block) = len(ca), ca[0].shape
    width = n_blocks * block
    tile = tile_of(rows, 640, 16)
    first = first_row // tile
    slab = pl.BlockSpec((tile, block), lambda i, s: (i, 0))
    whole = pl.BlockSpec((width, width), lambda i, s: (0, 0))

    def out_rows(columns):
        return pl.BlockSpec((tile, columns), lambda i, s: (first + i, 0))

    shapes = (
        jax.ShapeDtypeStruct((row_len, 2 * width), BF16),
        jax.ShapeDtypeStruct((row_len, 4 * width), F8),
        jax.ShapeDtypeStruct((row_len, 1), F32),
        jax.ShapeDtypeStruct((row_len, block), BF16),
        jax.ShapeDtypeStruct((row_len, block), BF16),
        jax.ShapeDtypeStruct(rhs.shape, F32),
        jax.ShapeDtypeStruct((1, rhs_len), F32),
    )
    n_in = 3 + 2 * n_blocks + 4
    *kept_out, sums = pl.pallas_call(
        functools.partial(factors_kernel, n_blocks, block, first_row, len(kept)),
        grid_spec=pltpu.PrefetchScalarGridSpec(
            num_scalar_prefetch=1,
            grid=(rows // tile,),
            in_specs=[
                out_rows(rhs_len),
                pl.BlockSpec((2 * width, rhs_len), lambda i, s: (0, 0)),
            ]
            + [slab] * (2 * n_blocks)
            + [whole] * 4
            + [pl.BlockSpec(memory_space=pl.ANY)] * len(kept),
            out_specs=[out_rows(s.shape[1]) for s in shapes[:-1]]
            + [pl.BlockSpec((1, rhs_len), lambda i, s: (0, 0))],
            scratch_shapes=[pltpu.VMEM((width, width), BF16)] * 4
            + [pltpu.VMEM((tile, width), F32)] * 2
            + [pltpu.VMEM((2 * width, rhs_len), BF16)]
            + [pltpu.VMEM((4 * width, rhs_len), F8)],
        ),
        out_shape=shapes,
        input_output_aliases={n_in + i: i for i in range(len(kept))},
        cost_estimate=cost_of(rows * (10 * width * width + 6 * width * rhs_len), rows * 8192),
        name="factors",
    )(scalars, rhs, rhs_upper, *ca, *cb, inv_a, inv_b, w_ab, w_ba, *kept)
    return kept_out, sums


def column_cuts(size):
    units = size // LANES
    if size % LANES or units < 6:
        return [0, size]
    return [0, units * 4 // 5 * LANES, size]


def tile_of(size, most, unit):
    for count in range(1, size // unit + 1):
        if size % (count * unit) == 0 and size // count <= most:
            return size // count
    return unit


def matrix_kernel(block, first_col, n_kept, scalars, a_ref, high, small, scale, upper, fa, fb, *refs):
    out_ref, token_ref, uh, us = refs[n_kept:]
    token_ref[...] = jnp.zeros_like(token_ref)

    @pl.when(pl.program_id(0) == 0)
    def _():
        prepare(upper, uh, us)

    update = dot(high[...], uh[...]) + dot(small[...], us[...]) * scale[...]
    out_ref[...] = (a_ref[...] - update).astype(BF16)
    width = out_ref.shape[1]
    for slot, final in ((0, fa), (1, fb)):
        offset = scalars[3 + slot] - first_col

        @pl.when((scalars[5 + slot] > 0) & (offset >= 0) & (offset < width))
        def _(final=final, offset=offset):
            out_ref[:, pl.ds(pl.multiple_of(offset, block), block)] = final[...]


def update_matrix(matrix, high, small, scale, upper, fa, fb, scalars, first_col, block, kept):
    rows, cols = matrix.shape
    depth, width = upper.shape
    tm = tile_of(rows, 768, block)
    here = pl.BlockSpec(
        (pl.Element(tm), pl.Element(width)), lambda i, s: (i * tm, first_col)
    )
    left = pl.BlockSpec((tm, depth), lambda i, s: (i, 0))
    final = pl.BlockSpec((tm, block), lambda i, s: (i, 0))
    return pl.pallas_call(
        functools.partial(matrix_kernel, block, first_col, len(kept)),
        grid_spec=pltpu.PrefetchScalarGridSpec(
            num_scalar_prefetch=1,
            grid=(rows // tm,),
            in_specs=[
                here, left,
                pl.BlockSpec((tm, 2 * depth), lambda i, s: (i, 0)),
                pl.BlockSpec((tm, 1), lambda i, s: (i, 0)),
                pl.BlockSpec((depth, width), lambda i, s: (0, 0)),
                final, final,
            ]
            + [pl.BlockSpec(memory_space=pl.ANY)] * len(kept),
            out_specs=[here, pl.BlockSpec((8, LANES), lambda i, s: (0, 0))],
            scratch_shapes=[
                pltpu.VMEM((depth, width), BF16), pltpu.VMEM((2 * depth, width), F8)
            ],
        ),
        out_shape=[
            jax.ShapeDtypeStruct((rows, cols), BF16),
            jax.ShapeDtypeStruct((8, LANES), F32),
        ],
        input_output_aliases={8: 0} if kept else {},
        cost_estimate=cost_of(3 * rows * depth * width, rows * width * 8),
        name="update_matrix",
    )(scalars, matrix, high, small, scale, upper, fa, fb, *kept)


def on_device(matrix, rhs, pivot_inverses, panel_order):
    row_count, col_count = lax.axis_size("row"), lax.axis_size("col")
    width = pivot_inverses.shape[1]
    block = width // row_count
    groups = col_count // row_count
    row_len, col_len = matrix.shape
    total_rows = row_len * row_count
    rhs_len = rhs.shape[1]
    col_index = lax.axis_index("col")
    own, group = lax.rem(col_index, row_count), lax.div(col_index, row_count)
    a, b = panel_order[0], panel_order[1]
    count = jnp.uint32(groups)
    unsigned = [p.astype(jnp.uint32) for p in (a, b)]
    places = [lax.rem(p, count).astype(jnp.int32) for p in unsigned]
    owns = [group == place for place in places]
    offsets = [lax.div(p, count).astype(jnp.int32) * block for p in unsigned]
    cut = functools.partial(lax.dynamic_slice, allow_negative_indices=False)
    masks = [0]
    bits = [row_count >> (k + 1) for k in range(row_count.bit_length() - 1)]
    for bit in bits:
        masks = masks + [m ^ bit for m in masks]

    def after(piece, event):
        return lax.optimization_barrier((piece, event))[0]

    def from_owner(piece, which, event=None):
        chosen = piece
        for step in range(1, groups):
            moved = lax.ppermute(
                piece, "col",
                [(i, (i + step * row_count) % col_count) for i in range(col_count)],
            )
            if event is not None:
                moved = after(moved, event)
            sender = lax.rem(group - step + groups, groups)
            chosen = jnp.where(sender == places[which], moved, chosen)
        return chosen

    def spread(pieces, bits):
        for bit in bits:
            swap = [(i, i ^ bit) for i in range(col_count)]
            pieces = pieces + [lax.ppermute(p, "col", swap) for p in pieces]
        return pieces

    parts = 3 if row_len % (3 * 32) == 0 else 1
    part = row_len // parts
    pieces = [
        cut(matrix, (h * part, offset), (part, block))
        for h in range(parts)
        for offset in offsets
    ]

    def rows_of(array):
        return [cut(array, (p * block, 0), (block, array.shape[1])) for p in (a, b)]

    cross = [
        cut(matrix, (a * block, offsets[1]), (block, block)),
        cut(matrix, (b * block, offsets[0]), (block, block)),
    ]
    rhs_rows = rows_of(rhs)
    pieces = after(pieces, (rhs_rows, cross))
    gather = functools.partial(lax.all_gather, axis_name="row", axis=0, tiled=True)
    head = gather(
        jnp.concatenate(
            [jnp.concatenate([c, r], axis=1) for r, c in zip(rhs_rows, cross)], axis=0
        )
    )
    aligned = block % LANES == 0 and col_len % LANES == 0 and rhs_len % LANES == 0
    cuts = column_cuts(col_len)
    panel_rows = after(rows_of(matrix), pieces[:2])
    strips = [
        jnp.concatenate([r[:, lo:hi] for r in panel_rows], axis=0)
        for lo, hi in zip(cuts, cuts[1:])
    ]
    uppers = [gather(strip) for strip in strips]

    chosen = [from_owner(p, n % 2) for n, p in enumerate(pieces[:3])]
    far, last = bits[:-1], bits[-1:]
    slabs = [spread([piece], far) for piece in chosen[:2]]
    head = after(head, [slab[-1] for slab in slabs])
    crossing, rhs_upper = head[:, :block], head[:, block:]
    crossed = crossing.reshape(row_count, 2, block, block)
    w_ab = from_owner(crossed[:, 0].reshape(width, block), 1)
    w_ba = from_owner(crossed[:, 1].reshape(width, block), 0)
    pieces[3:4] = after(pieces[3:4], crossing)
    pieces[4:] = after(pieces[4:], (w_ab, w_ba))
    chosen += [from_owner(p, 1) for p in pieces[3:4]]
    chosen[3:] = after(chosen[3:], (w_ab, w_ba))
    w_ab, w_ba = spread([w_ab], far), spread([w_ba], far)
    slabs += [spread([piece], far) for piece in chosen[2:]]
    w_ab, w_ba = [jnp.concatenate(spread(w, last), axis=1) for w in (w_ab, w_ba)]

    inverses = [
        jnp.concatenate(
            [
                cut(pivot_inverses[s], ((own ^ m) * block, 0), (block, width))
                for m in masks
            ],
            axis=0,
        )
        for s in range(2)
    ]

    tokens = []
    if aligned:
        scalars = jnp.stack(
            [a, b, own, offsets[0], offsets[1]] + [o.astype(jnp.int32) for o in owns]
        ).astype(jnp.int32)
        kept, all_sums = (), []
        for h in range(parts):
            pair = slabs[2 * h : 2 * h + 2]
            if h:
                pair = after(pair, all_sums[h - 1])
            kept, sums = factors(
                rhs, rhs_upper, *[spread(slab, last) for slab in pair], *inverses,
                w_ab, w_ba, scalars, h * part, kept,
            )
            all_sums.append(sums)
            if not h:
                slabs += [
                    spread([from_owner(p, n % 2, sums)], far)
                    for n, p in enumerate(pieces[4:])
                ]
        high, small, scale, fa, fb, new_rhs = kept
        out = ()
        for first_col, upper in zip(cuts, uppers):
            *out, token = update_matrix(
                matrix, high, small, scale, upper, fa, fb, scalars, first_col, block, out
            )
            tokens.append(token)
        factored, sums = out[0], functools.reduce(jnp.add, all_sums)[0]
    else:
        slabs += [
            spread([from_owner(p, n % 2)], far) for n, p in enumerate(pieces[4:])
        ]
        slabs = [spread(slab, last) for slab in slabs]
        row_block = (jnp.arange(row_len, dtype=jnp.int32) // block)[:, None]
        ca, cb = [
            jnp.concatenate(
                [jnp.concatenate(slabs[2 * h + s], axis=1) for h in range(parts)], axis=0
            )
            for s in range(2)
        ]
        m_a, new_b, m_b, left_a, left_b = factors_tile(
            ca, cb, row_block, a, b, *inverses, split(w_ab),
            split(dot2(split(w_ba), inverses[0])),
        )
        left = split(
            jnp.stack(
                [x.reshape(row_len, row_count, block) for x in (left_a, left_b)], axis=2
            ).reshape(row_len, 2 * width)
        )
        new_rhs = rhs - dot3(left, split(rhs_upper))
        sums = jnp.sum(new_rhs * new_rhs, axis=0)
        current = matrix - dot3(left, split(jnp.concatenate(uppers, axis=1)))
        in_a, in_b = row_block == a, row_block == b
        mine = [
            lax.dynamic_slice_in_dim(m, own * block, block, 1) for m in (m_a, m_b)
        ]
        final = (
            jnp.where(in_a, ca[:, :block], mine[0]),
            jnp.where(in_a, cb[:, :block], jnp.where(in_b, new_b[:, :block], mine[1])),
        )
        for values, offset, is_owner in zip(final, offsets, owns):
            old = lax.dynamic_slice_in_dim(current, offset, block, 1)
            current = lax.dynamic_update_slice_in_dim(
                current, jnp.where(is_owner, values, old), offset, 1
            )
        factored = current.astype(BF16)
    totals = sums
    for k in range(row_count.bit_length() - 1):
        moved = lax.ppermute(totals, "row", [(i, i ^ 1 << k) for i in range(row_count)])
        totals = totals + moved
    if len(tokens) > 1:
        totals = totals + tokens[0][0, 0]
    rhs_norms = jnp.sqrt(totals / total_rows + 1e-06)
    return factored, new_rhs, rhs_norms


def solution(mesh):
    in_specs = (P("row", "col"), P("row", "col"), P(), P())
    out_specs = (P("row", "col"), P("row", "col"), P("col"))
    return jax.shard_map(
        on_device, mesh=mesh, in_specs=in_specs, out_specs=out_specs, check_vma=False
    )
```

```python
import functools

import jax
import jax.numpy as jnp
from jax import lax
from jax.experimental import pallas as pl
from jax.experimental.pallas import tpu as pltpu
from jax.sharding import PartitionSpec as P

LANES = 128
F32 = jnp.float32
BF16 = jnp.bfloat16
F8 = jnp.float8_e4m3fn
TOP, LOW_UP = 224.0, 2.0**8


def cost_of(products, size):
    return pl.CostEstimate(flops=2 * products, bytes_accessed=size, transcendentals=0)


def split(values):
    high = values.astype(BF16)
    return high, (values - high.astype(F32)).astype(BF16)


def dot(first, second):
    return jnp.dot(first, second, preferred_element_type=F32)


def dot3(first, second):
    (fh, fl), (sh, sl) = first, second
    return dot(fh, sh) + dot(fh, sl) + dot(fl, sh)


def dot2(first, second):
    fh, fl = first
    return dot(fh, second) + dot(fl, second)


def factors_tile(ca, cb, row_block, a, b, inv_a, inv_b, w_ab, pivot_rows):
    in_a, in_b = row_block == a, row_block == b
    m_a = dot2(split(ca), inv_a)
    new_b = cb - dot3(split(m_a), w_ab)
    m_b = dot2(split(new_b), inv_b)
    left_a = m_a - dot3(split(m_b), pivot_rows)
    left_a = jnp.where(in_a, 0.0, jnp.where(in_b, m_a, left_a))
    left_b = jnp.where(in_a | in_b, 0.0, m_b)
    return m_a, new_b, m_b, left_a, left_b


def prepare(upper, high, small, scale):
    depth = upper.shape[0]
    step = depth // 4
    top = jnp.full(scale.shape, 1e-30, F32)
    for first in range(0, depth, step):
        size = jnp.abs(upper[first : first + step, :])
        top = jnp.maximum(top, jnp.max(size, axis=0, keepdims=True))
    up = TOP / top
    scale[...] = top / (TOP * LOW_UP)

    def some(k, carry):
        here = pl.ds(pl.multiple_of(k * step, step), step)
        values = upper[here, :]
        rounded = values.astype(BF16)
        high[here, :] = rounded
        rest = values - rounded.astype(F32)
        small[here, :] = (rest * (up * LOW_UP)).astype(F8)
        there = pl.ds(pl.multiple_of(depth + k * step, step), step)
        small[there, :] = (values * up).astype(F8)
        return carry

    lax.fori_loop(0, 4, some, 0)


def factors_kernel(
    n_blocks, block, first_row, n_kept, scalars, *refs
):
    rhs_ref, upper_ref, *refs = refs
    ca_refs, cb_refs = refs[:n_blocks], refs[n_blocks : 2 * n_blocks]
    inv_a, inv_b, w_ab, w_ba = refs[2 * n_blocks : 2 * n_blocks + 4]
    out = refs[2 * n_blocks + 4 + n_kept :]
    high_ref, small_ref, scale_ref, fa_ref, fb_ref, new_rhs_ref, sums_ref, *scratch = out
    wh, wl, ph, pll, ma_s, mb_s, uh, us, column_scale = scratch
    a, b, own = scalars[0], scalars[1], scalars[2]

    @pl.when(pl.program_id(0) == 0)
    def _():
        wh[...], wl[...] = split(w_ab[...])
        ph[...], pll[...] = split(dot2(split(w_ba[...]), inv_a[...]))
        prepare(upper_ref, uh, us, column_scale)
        sums_ref[...] = jnp.zeros_like(sums_ref)

    rows = high_ref.shape[0]
    start = first_row + pl.program_id(0) * rows
    row_block = (start + lax.broadcasted_iota(jnp.int32, (rows, 1), 0)) // block
    ca = jnp.concatenate([r[...] for r in ca_refs], axis=1)
    cb = jnp.concatenate([r[...] for r in cb_refs], axis=1)
    m_a, new_b, m_b, left_a, left_b = factors_tile(
        ca, cb, row_block, a, b, inv_a[...], inv_b[...],
        (wh[...], wl[...]), (ph[...], pll[...]),
    )
    top = jnp.maximum(
        jnp.max(jnp.maximum(jnp.abs(left_a), jnp.abs(left_b)), axis=1, keepdims=True),
        1e-30,
    )
    up = TOP / top
    scale_ref[...] = top / TOP
    depth = high_ref.shape[1]
    for left, shift in ((left_a, 0), (left_b, 1)):
        high = left.astype(BF16)
        rest = left - high.astype(F32)
        small_high = (left * up).astype(F8)
        small_low = (rest * (up * LOW_UP)).astype(F8)
        for r in range(n_blocks):
            start, here = (2 * r + shift) * block, slice(r * block, (r + 1) * block)
            high_ref[:, pl.ds(start, block)] = high[:, here]
            small_ref[:, pl.ds(start, block)] = small_high[:, here]
            small_ref[:, pl.ds(depth + start, block)] = small_low[:, here]
    ma_s[...], mb_s[...] = m_a, m_b
    mine = pl.ds(pl.multiple_of(own * block, block), block)
    in_a, in_b = row_block == a, row_block == b
    fa_ref[...] = jnp.where(in_a, ca_refs[0][...], ma_s[:, mine]).astype(BF16)
    fb_ref[...] = jnp.where(
        in_a, cb_refs[0][...], jnp.where(in_b, new_b[:, :block], mb_s[:, mine])
    ).astype(BF16)
    small = dot(small_ref[...], us[...]) * (scale_ref[...] * column_scale[...])
    new_rhs = rhs_ref[...] - (dot(high_ref[...], uh[...]) + small)
    new_rhs_ref[...] = new_rhs
    sums_ref[...] += jnp.sum(new_rhs * new_rhs, axis=0, keepdims=True)


def factors(
    rhs, rhs_upper, ca, cb, inv_a, inv_b, w_ab, w_ba, scalars, first_row, kept
):
    row_len, rhs_len = rhs.shape
    n_blocks, (rows, block) = len(ca), ca[0].shape
    width = n_blocks * block
    tile = tile_of(rows, 640, 16)
    first = first_row // tile
    slab = pl.BlockSpec((tile, block), lambda i, s: (i, 0))
    whole = pl.BlockSpec((width, width), lambda i, s: (0, 0))

    def out_rows(columns):
        return pl.BlockSpec((tile, columns), lambda i, s: (first + i, 0))

    shapes = (
        jax.ShapeDtypeStruct((row_len, 2 * width), BF16),
        jax.ShapeDtypeStruct((row_len, 4 * width), F8),
        jax.ShapeDtypeStruct((row_len, 1), F32),
        jax.ShapeDtypeStruct((row_len, block), BF16),
        jax.ShapeDtypeStruct((row_len, block), BF16),
        jax.ShapeDtypeStruct(rhs.shape, F32),
        jax.ShapeDtypeStruct((1, rhs_len), F32),
    )
    n_in = 3 + 2 * n_blocks + 4
    *kept_out, sums = pl.pallas_call(
        functools.partial(factors_kernel, n_blocks, block, first_row, len(kept)),
        grid_spec=pltpu.PrefetchScalarGridSpec(
            num_scalar_prefetch=1,
            grid=(rows // tile,),
            in_specs=[
                out_rows(rhs_len),
                pl.BlockSpec((2 * width, rhs_len), lambda i, s: (0, 0)),
            ]
            + [slab] * (2 * n_blocks)
            + [whole] * 4
            + [pl.BlockSpec(memory_space=pl.ANY)] * len(kept),
            out_specs=[out_rows(s.shape[1]) for s in shapes[:-1]]
            + [pl.BlockSpec((1, rhs_len), lambda i, s: (0, 0))],
            scratch_shapes=[pltpu.VMEM((width, width), BF16)] * 4
            + [pltpu.VMEM((tile, width), F32)] * 2
            + [pltpu.VMEM((2 * width, rhs_len), BF16)]
            + [pltpu.VMEM((4 * width, rhs_len), F8)]
            + [pltpu.VMEM((1, rhs_len), F32)],
        ),
        out_shape=shapes,
        input_output_aliases={n_in + i: i for i in range(len(kept))},
        cost_estimate=cost_of(rows * (10 * width * width + 6 * width * rhs_len), rows * 8192),
        name="factors",
    )(scalars, rhs, rhs_upper, *ca, *cb, inv_a, inv_b, w_ab, w_ba, *kept)
    return kept_out, sums


def column_cuts(size):
    units = size // LANES
    if size % LANES or units < 6:
        return [0, size]
    return [0, units * 4 // 5 * LANES, size]


def tile_of(size, most, unit):
    for count in range(1, size // unit + 1):
        if size % (count * unit) == 0 and size // count <= most:
            return size // count
    return unit


def matrix_kernel(block, first_col, n_kept, scalars, a_ref, high, small, scale, upper, fa, fb, *refs):
    out_ref, token_ref, uh, us, column_scale = refs[n_kept:]
    token_ref[...] = jnp.zeros_like(token_ref)

    @pl.when(pl.program_id(0) == 0)
    def _():
        prepare(upper, uh, us, column_scale)

    update = dot(high[...], uh[...]) + dot(small[...], us[...]) * (
        scale[...] * column_scale[...]
    )
    out_ref[...] = (a_ref[...] - update).astype(BF16)
    width = out_ref.shape[1]
    for slot, final in ((0, fa), (1, fb)):
        offset = scalars[3 + slot] - first_col

        @pl.when((scalars[5 + slot] > 0) & (offset >= 0) & (offset < width))
        def _(final=final, offset=offset):
            out_ref[:, pl.ds(pl.multiple_of(offset, block), block)] = final[...]


def update_matrix(matrix, high, small, scale, upper, fa, fb, scalars, first_col, block, kept):
    rows, cols = matrix.shape
    depth, width = upper.shape
    tm = tile_of(rows, 768, block)
    here = pl.BlockSpec(
        (pl.Element(tm), pl.Element(width)), lambda i, s: (i * tm, first_col)
    )
    left = pl.BlockSpec((tm, depth), lambda i, s: (i, 0))
    final = pl.BlockSpec((tm, block), lambda i, s: (i, 0))
    return pl.pallas_call(
        functools.partial(matrix_kernel, block, first_col, len(kept)),
        grid_spec=pltpu.PrefetchScalarGridSpec(
            num_scalar_prefetch=1,
            grid=(rows // tm,),
            in_specs=[
                here, left,
                pl.BlockSpec((tm, 2 * depth), lambda i, s: (i, 0)),
                pl.BlockSpec((tm, 1), lambda i, s: (i, 0)),
                pl.BlockSpec((depth, width), lambda i, s: (0, 0)),
                final, final,
            ]
            + [pl.BlockSpec(memory_space=pl.ANY)] * len(kept),
            out_specs=[here, pl.BlockSpec((8, LANES), lambda i, s: (0, 0))],
            scratch_shapes=[
                pltpu.VMEM((depth, width), BF16),
                pltpu.VMEM((2 * depth, width), F8),
                pltpu.VMEM((1, width), F32),
            ],
        ),
        out_shape=[
            jax.ShapeDtypeStruct((rows, cols), BF16),
            jax.ShapeDtypeStruct((8, LANES), F32),
        ],
        input_output_aliases={8: 0} if kept else {},
        cost_estimate=cost_of(3 * rows * depth * width, rows * width * 8),
        name="update_matrix",
    )(scalars, matrix, high, small, scale, upper, fa, fb, *kept)


def on_device(matrix, rhs, pivot_inverses, panel_order):
    row_count, col_count = lax.axis_size("row"), lax.axis_size("col")
    width = pivot_inverses.shape[1]
    block = width // row_count
    groups = col_count // row_count
    row_len, col_len = matrix.shape
    total_rows = row_len * row_count
    rhs_len = rhs.shape[1]
    col_index = lax.axis_index("col")
    own, group = lax.rem(col_index, row_count), lax.div(col_index, row_count)
    a, b = panel_order[0], panel_order[1]
    count = jnp.uint32(groups)
    unsigned = [p.astype(jnp.uint32) for p in (a, b)]
    places = [lax.rem(p, count).astype(jnp.int32) for p in unsigned]
    owns = [group == place for place in places]
    offsets = [lax.div(p, count).astype(jnp.int32) * block for p in unsigned]
    cut = functools.partial(lax.dynamic_slice, allow_negative_indices=False)
    masks = [0]
    bits = [row_count >> (k + 1) for k in range(row_count.bit_length() - 1)]
    for bit in bits:
        masks = masks + [m ^ bit for m in masks]

    def after(piece, event):
        return lax.optimization_barrier((piece, event))[0]

    def from_owner(piece, which, event=None):
        chosen = piece
        for step in range(1, groups):
            moved = lax.ppermute(
                piece, "col",
                [(i, (i + step * row_count) % col_count) for i in range(col_count)],
            )
            if event is not None:
                moved = after(moved, event)
            sender = lax.rem(group - step + groups, groups)
            chosen = jnp.where(sender == places[which], moved, chosen)
        return chosen

    def spread(pieces, bits):
        for bit in bits:
            swap = [(i, i ^ bit) for i in range(col_count)]
            pieces = pieces + [lax.ppermute(p, "col", swap) for p in pieces]
        return pieces

    parts = 3 if row_len % (3 * 32) == 0 else 1
    part = row_len // parts
    pieces = [
        cut(matrix, (h * part, offset), (part, block))
        for h in range(parts)
        for offset in offsets
    ]

    def rows_of(array):
        return [cut(array, (p * block, 0), (block, array.shape[1])) for p in (a, b)]

    cross = [
        cut(matrix, (a * block, offsets[1]), (block, block)),
        cut(matrix, (b * block, offsets[0]), (block, block)),
    ]
    rhs_rows = rows_of(rhs)
    pieces = after(pieces, (rhs_rows, cross))
    gather = functools.partial(lax.all_gather, axis_name="row", axis=0, tiled=True)
    head = gather(
        jnp.concatenate(
            [jnp.concatenate([c, r], axis=1) for r, c in zip(rhs_rows, cross)], axis=0
        )
    )
    aligned = block % LANES == 0 and col_len % LANES == 0 and rhs_len % LANES == 0
    cuts = column_cuts(col_len)
    panel_rows = after(rows_of(matrix), pieces[:2])
    strips = [
        jnp.concatenate([r[:, lo:hi] for r in panel_rows], axis=0)
        for lo, hi in zip(cuts, cuts[1:])
    ]
    uppers = [gather(strip) for strip in strips]

    chosen = [from_owner(p, n % 2) for n, p in enumerate(pieces[:3])]
    far, last = bits[:-1], bits[-1:]
    slabs = [spread([piece], far) for piece in chosen[:2]]
    head = after(head, [slab[-1] for slab in slabs])
    crossing, rhs_upper = head[:, :block], head[:, block:]
    crossed = crossing.reshape(row_count, 2, block, block)
    w_ab = from_owner(crossed[:, 0].reshape(width, block), 1)
    w_ba = from_owner(crossed[:, 1].reshape(width, block), 0)
    pieces[3:4] = after(pieces[3:4], crossing)
    pieces[4:] = after(pieces[4:], (w_ab, w_ba))
    chosen += [from_owner(p, 1) for p in pieces[3:4]]
    chosen[3:] = after(chosen[3:], (w_ab, w_ba))
    w_ab, w_ba = spread([w_ab], far), spread([w_ba], far)
    slabs += [spread([piece], far) for piece in chosen[2:]]
    w_ab, w_ba = [jnp.concatenate(spread(w, last), axis=1) for w in (w_ab, w_ba)]

    inverses = [
        jnp.concatenate(
            [
                cut(pivot_inverses[s], ((own ^ m) * block, 0), (block, width))
                for m in masks
            ],
            axis=0,
        )
        for s in range(2)
    ]

    tokens = []
    if aligned:
        scalars = jnp.stack(
            [a, b, own, offsets[0], offsets[1]] + [o.astype(jnp.int32) for o in owns]
        ).astype(jnp.int32)
        kept, all_sums = (), []
        for h in range(parts):
            pair = slabs[2 * h : 2 * h + 2]
            if h:
                pair = after(pair, all_sums[h - 1])
            kept, sums = factors(
                rhs, rhs_upper, *[spread(slab, last) for slab in pair], *inverses,
                w_ab, w_ba, scalars, h * part, kept,
            )
            all_sums.append(sums)
            if not h:
                slabs += [
                    spread([from_owner(p, n % 2, sums)], far)
                    for n, p in enumerate(pieces[4:])
                ]
        high, small, scale, fa, fb, new_rhs = kept
        out = ()
        for first_col, upper in zip(cuts, uppers):
            *out, token = update_matrix(
                matrix, high, small, scale, upper, fa, fb, scalars, first_col, block, out
            )
            tokens.append(token)
        factored, sums = out[0], functools.reduce(jnp.add, all_sums)[0]
    else:
        slabs += [
            spread([from_owner(p, n % 2)], far) for n, p in enumerate(pieces[4:])
        ]
        slabs = [spread(slab, last) for slab in slabs]
        row_block = (jnp.arange(row_len, dtype=jnp.int32) // block)[:, None]
        ca, cb = [
            jnp.concatenate(
                [jnp.concatenate(slabs[2 * h + s], axis=1) for h in range(parts)], axis=0
            )
            for s in range(2)
        ]
        m_a, new_b, m_b, left_a, left_b = factors_tile(
            ca, cb, row_block, a, b, *inverses, split(w_ab),
            split(dot2(split(w_ba), inverses[0])),
        )
        left = split(
            jnp.stack(
                [x.reshape(row_len, row_count, block) for x in (left_a, left_b)], axis=2
            ).reshape(row_len, 2 * width)
        )
        new_rhs = rhs - dot3(left, split(rhs_upper))
        sums = jnp.sum(new_rhs * new_rhs, axis=0)
        current = matrix - dot3(left, split(jnp.concatenate(uppers, axis=1)))
        in_a, in_b = row_block == a, row_block == b
        mine = [
            lax.dynamic_slice_in_dim(m, own * block, block, 1) for m in (m_a, m_b)
        ]
        final = (
            jnp.where(in_a, ca[:, :block], mine[0]),
            jnp.where(in_a, cb[:, :block], jnp.where(in_b, new_b[:, :block], mine[1])),
        )
        for values, offset, is_owner in zip(final, offsets, owns):
            old = lax.dynamic_slice_in_dim(current, offset, block, 1)
            current = lax.dynamic_update_slice_in_dim(
                current, jnp.where(is_owner, values, old), offset, 1
            )
        factored = current.astype(BF16)
    totals = sums
    for k in range(row_count.bit_length() - 1):
        moved = lax.ppermute(totals, "row", [(i, i ^ 1 << k) for i in range(row_count)])
        totals = totals + moved
    if len(tokens) > 1:
        totals = totals + tokens[0][0, 0]
    rhs_norms = jnp.sqrt(totals / total_rows + 1e-06)
    return factored, new_rhs, rhs_norms


def solution(mesh):
    in_specs = (P("row", "col"), P("row", "col"), P(), P())
    out_specs = (P("row", "col"), P("row", "col"), P("col"))
    return jax.shard_map(
        on_device, mesh=mesh, in_specs=in_specs, out_specs=out_specs, check_vma=False
    )
```

```python
import functools

import jax
import jax.numpy as jnp
from jax import lax
from jax.experimental import pallas as pl
from jax.experimental.pallas import tpu as pltpu
from jax.sharding import PartitionSpec as P

LANES = 128
F32 = jnp.float32
BF16 = jnp.bfloat16
F8 = jnp.float8_e4m3fn
TOP, LOW_UP = 224.0, 2.0**8


def cost_of(products, size):
    return pl.CostEstimate(flops=2 * products, bytes_accessed=size, transcendentals=0)


def split(values):
    high = values.astype(BF16)
    return high, (values - high.astype(F32)).astype(BF16)


def dot(first, second):
    return jnp.dot(first, second, preferred_element_type=F32)


def dot3(first, second):
    (fh, fl), (sh, sl) = first, second
    return dot(fh, sh) + dot(fh, sl) + dot(fl, sh)


def dot2(first, second):
    fh, fl = first
    return dot(fh, second) + dot(fl, second)


def factors_tile(ca, cb, row_block, a, b, inv_a, inv_b, w_ab, pivot_rows):
    in_a, in_b = row_block == a, row_block == b
    m_a = dot2(split(ca), inv_a)
    new_b = cb - dot3(split(m_a), w_ab)
    m_b = dot2(split(new_b), inv_b)
    left_a = m_a - dot3(split(m_b), pivot_rows)
    left_a = jnp.where(in_a, 0.0, jnp.where(in_b, m_a, left_a))
    left_b = jnp.where(in_a | in_b, 0.0, m_b)
    return m_a, new_b, m_b, left_a, left_b


def prepare(upper, high, small, scale):
    depth = upper.shape[0]
    step = depth // 4
    top = jnp.full(scale.shape, 1e-30, F32)
    for first in range(0, depth, step):
        size = jnp.abs(upper[first : first + step, :])
        top = jnp.maximum(top, jnp.max(size, axis=0, keepdims=True))
    up = TOP / top
    scale[...] = top / (TOP * LOW_UP)

    def some(k, carry):
        here = pl.ds(pl.multiple_of(k * step, step), step)
        values = upper[here, :]
        rounded = values.astype(BF16)
        high[here, :] = rounded
        rest = values - rounded.astype(F32)
        small[here, :] = (rest * (up * LOW_UP)).astype(F8)
        there = pl.ds(pl.multiple_of(depth + k * step, step), step)
        small[there, :] = (values * up).astype(F8)
        return carry

    lax.fori_loop(0, 4, some, 0)


def factors_kernel(
    n_blocks, block, first_row, n_kept, scalars, *refs
):
    rhs_ref, upper_ref, *refs = refs
    ca_refs, cb_refs = refs[:n_blocks], refs[n_blocks : 2 * n_blocks]
    inv_a, inv_b, w_ab, w_ba = refs[2 * n_blocks : 2 * n_blocks + 4]
    out = refs[2 * n_blocks + 4 + n_kept :]
    high_ref, small_ref, scale_ref, fa_ref, fb_ref, new_rhs_ref, sums_ref, *scratch = out
    wh, wl, ph, pll, ma_s, mb_s, uh, us, column_scale = scratch
    a, b, own = scalars[0], scalars[1], scalars[2]

    @pl.when(pl.program_id(0) == 0)
    def _():
        wh[...], wl[...] = split(w_ab[...])
        ph[...], pll[...] = split(dot2(split(w_ba[...]), inv_a[...]))
        prepare(upper_ref, uh, us, column_scale)
        sums_ref[...] = jnp.zeros_like(sums_ref)

    rows = high_ref.shape[0]
    start = first_row + pl.program_id(0) * rows
    row_block = (start + lax.broadcasted_iota(jnp.int32, (rows, 1), 0)) // block
    ca = jnp.concatenate([r[...] for r in ca_refs], axis=1)
    cb = jnp.concatenate([r[...] for r in cb_refs], axis=1)
    m_a, new_b, m_b, left_a, left_b = factors_tile(
        ca, cb, row_block, a, b, inv_a[...], inv_b[...],
        (wh[...], wl[...]), (ph[...], pll[...]),
    )
    top = jnp.maximum(
        jnp.max(jnp.maximum(jnp.abs(left_a), jnp.abs(left_b)), axis=1, keepdims=True),
        1e-30,
    )
    up = TOP / top
    scale_ref[...] = top / TOP
    depth = high_ref.shape[1]
    for left, shift in ((left_a, 0), (left_b, 1)):
        high = left.astype(BF16)
        rest = left - high.astype(F32)
        small_high = (left * up).astype(F8)
        small_low = (rest * (up * LOW_UP)).astype(F8)
        for r in range(n_blocks):
            start, here = (2 * r + shift) * block, slice(r * block, (r + 1) * block)
            high_ref[:, pl.ds(start, block)] = high[:, here]
            small_ref[:, pl.ds(start, block)] = small_high[:, here]
            small_ref[:, pl.ds(depth + start, block)] = small_low[:, here]
    ma_s[...], mb_s[...] = m_a, m_b
    mine = pl.ds(pl.multiple_of(own * block, block), block)
    in_a, in_b = row_block == a, row_block == b
    fa_ref[...] = jnp.where(in_a, ca_refs[0][...], ma_s[:, mine]).astype(BF16)
    fb_ref[...] = jnp.where(
        in_a, cb_refs[0][...], jnp.where(in_b, new_b[:, :block], mb_s[:, mine])
    ).astype(BF16)
    small = dot(small_ref[...], us[...]) * (scale_ref[...] * column_scale[...])
    new_rhs = rhs_ref[...] - (dot(high_ref[...], uh[...]) + small)
    new_rhs_ref[...] = new_rhs
    sums_ref[...] += jnp.sum(new_rhs * new_rhs, axis=0, keepdims=True)


def factors(
    rhs, rhs_upper, ca, cb, inv_a, inv_b, w_ab, w_ba, scalars, first_row, kept
):
    row_len, rhs_len = rhs.shape
    n_blocks, (rows, block) = len(ca), ca[0].shape
    width = n_blocks * block
    tile = tile_of(rows, 640, 16)
    first = first_row // tile
    slab = pl.BlockSpec((tile, block), lambda i, s: (i, 0))
    whole = pl.BlockSpec((width, width), lambda i, s: (0, 0))

    def out_rows(columns):
        return pl.BlockSpec((tile, columns), lambda i, s: (first + i, 0))

    shapes = (
        jax.ShapeDtypeStruct((row_len, 2 * width), BF16),
        jax.ShapeDtypeStruct((row_len, 4 * width), F8),
        jax.ShapeDtypeStruct((row_len, 1), F32),
        jax.ShapeDtypeStruct((row_len, block), BF16),
        jax.ShapeDtypeStruct((row_len, block), BF16),
        jax.ShapeDtypeStruct(rhs.shape, F32),
        jax.ShapeDtypeStruct((1, rhs_len), F32),
    )
    n_in = 3 + 2 * n_blocks + 4
    *kept_out, sums = pl.pallas_call(
        functools.partial(factors_kernel, n_blocks, block, first_row, len(kept)),
        grid_spec=pltpu.PrefetchScalarGridSpec(
            num_scalar_prefetch=1,
            grid=(rows // tile,),
            in_specs=[
                out_rows(rhs_len),
                pl.BlockSpec((2 * width, rhs_len), lambda i, s: (0, 0)),
            ]
            + [slab] * (2 * n_blocks)
            + [whole] * 4
            + [pl.BlockSpec(memory_space=pl.ANY)] * len(kept),
            out_specs=[out_rows(s.shape[1]) for s in shapes[:-1]]
            + [pl.BlockSpec((1, rhs_len), lambda i, s: (0, 0))],
            scratch_shapes=[pltpu.VMEM((width, width), BF16)] * 4
            + [pltpu.VMEM((tile, width), F32)] * 2
            + [pltpu.VMEM((2 * width, rhs_len), BF16)]
            + [pltpu.VMEM((4 * width, rhs_len), F8)]
            + [pltpu.VMEM((1, rhs_len), F32)],
        ),
        out_shape=shapes,
        input_output_aliases={n_in + i: i for i in range(len(kept))},
        cost_estimate=cost_of(rows * (10 * width * width + 6 * width * rhs_len), rows * 8192),
        name="factors",
    )(scalars, rhs, rhs_upper, *ca, *cb, inv_a, inv_b, w_ab, w_ba, *kept)
    return kept_out, sums


def column_cuts(size):
    units = size // LANES
    if size % LANES or units < 6:
        return [0, size]
    return [0, units * 4 // 5 * LANES, size]


def tile_of(size, most, unit):
    for count in range(1, size // unit + 1):
        if size % (count * unit) == 0 and size // count <= most:
            return size // count
    return unit


def matrix_kernel(block, first_col, n_kept, scalars, a_ref, high, small, scale, upper, fa, fb, *refs):
    out_ref, token_ref, uh, us, column_scale = refs[n_kept:]
    token_ref[...] = jnp.zeros_like(token_ref)

    @pl.when(pl.program_id(0) == 0)
    def _():
        prepare(upper, uh, us, column_scale)

    update = dot(high[...], uh[...]) + dot(small[...], us[...]) * (
        scale[...] * column_scale[...]
    )
    out_ref[...] = (a_ref[...] - update).astype(BF16)
    width = out_ref.shape[1]
    for slot, final in ((0, fa), (1, fb)):
        offset = scalars[3 + slot] - first_col

        @pl.when((scalars[5 + slot] > 0) & (offset >= 0) & (offset < width))
        def _(final=final, offset=offset):
            out_ref[:, pl.ds(pl.multiple_of(offset, block), block)] = final[...]


def update_matrix(matrix, high, small, scale, upper, fa, fb, scalars, first_col, block, kept):
    rows, cols = matrix.shape
    depth, width = upper.shape
    tm = tile_of(rows, 384 if 2 * width > cols else 768, block)
    here = pl.BlockSpec(
        (pl.Element(tm), pl.Element(width)), lambda i, s: (i * tm, first_col)
    )
    left = pl.BlockSpec((tm, depth), lambda i, s: (i, 0))
    final = pl.BlockSpec((tm, block), lambda i, s: (i, 0))
    return pl.pallas_call(
        functools.partial(matrix_kernel, block, first_col, len(kept)),
        grid_spec=pltpu.PrefetchScalarGridSpec(
            num_scalar_prefetch=1,
            grid=(rows // tm,),
            in_specs=[
                here, left,
                pl.BlockSpec((tm, 2 * depth), lambda i, s: (i, 0)),
                pl.BlockSpec((tm, 1), lambda i, s: (i, 0)),
                pl.BlockSpec((depth, width), lambda i, s: (0, 0)),
                final, final,
            ]
            + [pl.BlockSpec(memory_space=pl.ANY)] * len(kept),
            out_specs=[here, pl.BlockSpec((8, LANES), lambda i, s: (0, 0))],
            scratch_shapes=[
                pltpu.VMEM((depth, width), BF16),
                pltpu.VMEM((2 * depth, width), F8),
                pltpu.VMEM((1, width), F32),
            ],
        ),
        out_shape=[
            jax.ShapeDtypeStruct((rows, cols), BF16),
            jax.ShapeDtypeStruct((8, LANES), F32),
        ],
        input_output_aliases={8: 0} if kept else {},
        cost_estimate=cost_of(3 * rows * depth * width, rows * width * 8),
        name="update_matrix",
    )(scalars, matrix, high, small, scale, upper, fa, fb, *kept)


def on_device(matrix, rhs, pivot_inverses, panel_order):
    row_count, col_count = lax.axis_size("row"), lax.axis_size("col")
    width = pivot_inverses.shape[1]
    block = width // row_count
    groups = col_count // row_count
    row_len, col_len = matrix.shape
    total_rows = row_len * row_count
    rhs_len = rhs.shape[1]
    col_index = lax.axis_index("col")
    own, group = lax.rem(col_index, row_count), lax.div(col_index, row_count)
    a, b = panel_order[0], panel_order[1]
    count = jnp.uint32(groups)
    unsigned = [p.astype(jnp.uint32) for p in (a, b)]
    places = [lax.rem(p, count).astype(jnp.int32) for p in unsigned]
    owns = [group == place for place in places]
    offsets = [lax.div(p, count).astype(jnp.int32) * block for p in unsigned]
    cut = functools.partial(lax.dynamic_slice, allow_negative_indices=False)
    masks = [0]
    bits = [row_count >> (k + 1) for k in range(row_count.bit_length() - 1)]
    for bit in bits:
        masks = masks + [m ^ bit for m in masks]

    def after(piece, event):
        return lax.optimization_barrier((piece, event))[0]

    def from_owner(piece, which, event=None):
        chosen = piece
        for step in range(1, groups):
            moved = lax.ppermute(
                piece, "col",
                [(i, (i + step * row_count) % col_count) for i in range(col_count)],
            )
            if event is not None:
                moved = after(moved, event)
            sender = lax.rem(group - step + groups, groups)
            chosen = jnp.where(sender == places[which], moved, chosen)
        return chosen

    def spread(pieces, bits):
        for bit in bits:
            swap = [(i, i ^ bit) for i in range(col_count)]
            pieces = pieces + [lax.ppermute(p, "col", swap) for p in pieces]
        return pieces

    parts = 3 if row_len % (3 * 32) == 0 else 1
    part = row_len // parts
    pieces = [
        cut(matrix, (h * part, offset), (part, block))
        for h in range(parts)
        for offset in offsets
    ]

    def rows_of(array):
        return [cut(array, (p * block, 0), (block, array.shape[1])) for p in (a, b)]

    cross = [
        cut(matrix, (a * block, offsets[1]), (block, block)),
        cut(matrix, (b * block, offsets[0]), (block, block)),
    ]
    rhs_rows = rows_of(rhs)
    pieces = after(pieces, (rhs_rows, cross))
    gather = functools.partial(lax.all_gather, axis_name="row", axis=0, tiled=True)
    head = gather(
        jnp.concatenate(
            [jnp.concatenate([c, r], axis=1) for r, c in zip(rhs_rows, cross)], axis=0
        )
    )
    aligned = block % LANES == 0 and col_len % LANES == 0 and rhs_len % LANES == 0
    cuts = column_cuts(col_len)
    panel_rows = after(rows_of(matrix), pieces[:2])
    strips = [
        jnp.concatenate([r[:, lo:hi] for r in panel_rows], axis=0)
        for lo, hi in zip(cuts, cuts[1:])
    ]
    uppers = [gather(strip) for strip in strips]

    chosen = [from_owner(p, n % 2) for n, p in enumerate(pieces[:3])]
    far, last = bits[:-1], bits[-1:]
    slabs = [spread([piece], far) for piece in chosen[:2]]
    head = after(head, [slab[-1] for slab in slabs])
    crossing, rhs_upper = head[:, :block], head[:, block:]
    crossed = crossing.reshape(row_count, 2, block, block)
    w_ab = from_owner(crossed[:, 0].reshape(width, block), 1)
    w_ba = from_owner(crossed[:, 1].reshape(width, block), 0)
    pieces[3:4] = after(pieces[3:4], crossing)
    pieces[4:] = after(pieces[4:], (w_ab, w_ba))
    chosen += [from_owner(p, 1) for p in pieces[3:4]]
    chosen[3:] = after(chosen[3:], (w_ab, w_ba))
    w_ab, w_ba = spread([w_ab], far), spread([w_ba], far)
    slabs += [spread([piece], far) for piece in chosen[2:]]
    w_ab, w_ba = [jnp.concatenate(spread(w, last), axis=1) for w in (w_ab, w_ba)]

    inverses = [
        jnp.concatenate(
            [
                cut(pivot_inverses[s], ((own ^ m) * block, 0), (block, width))
                for m in masks
            ],
            axis=0,
        )
        for s in range(2)
    ]

    tokens = []
    if aligned:
        scalars = jnp.stack(
            [a, b, own, offsets[0], offsets[1]] + [o.astype(jnp.int32) for o in owns]
        ).astype(jnp.int32)
        kept, all_sums = (), []
        for h in range(parts):
            pair = slabs[2 * h : 2 * h + 2]
            if h:
                pair = after(pair, all_sums[h - 1])
            kept, sums = factors(
                rhs, rhs_upper, *[spread(slab, last) for slab in pair], *inverses,
                w_ab, w_ba, scalars, h * part, kept,
            )
            all_sums.append(sums)
            if not h:
                slabs += [
                    spread([from_owner(p, n % 2, sums)], far)
                    for n, p in enumerate(pieces[4:])
                ]
        high, small, scale, fa, fb, new_rhs = kept
        out = ()
        for first_col, upper in zip(cuts, uppers):
            *out, token = update_matrix(
                matrix, high, small, scale, upper, fa, fb, scalars, first_col, block, out
            )
            tokens.append(token)
        factored, sums = out[0], functools.reduce(jnp.add, all_sums)[0]
    else:
        slabs += [
            spread([from_owner(p, n % 2)], far) for n, p in enumerate(pieces[4:])
        ]
        slabs = [spread(slab, last) for slab in slabs]
        row_block = (jnp.arange(row_len, dtype=jnp.int32) // block)[:, None]
        ca, cb = [
            jnp.concatenate(
                [jnp.concatenate(slabs[2 * h + s], axis=1) for h in range(parts)], axis=0
            )
            for s in range(2)
        ]
        m_a, new_b, m_b, left_a, left_b = factors_tile(
            ca, cb, row_block, a, b, *inverses, split(w_ab),
            split(dot2(split(w_ba), inverses[0])),
        )
        left = split(
            jnp.stack(
                [x.reshape(row_len, row_count, block) for x in (left_a, left_b)], axis=2
            ).reshape(row_len, 2 * width)
        )
        new_rhs = rhs - dot3(left, split(rhs_upper))
        sums = jnp.sum(new_rhs * new_rhs, axis=0)
        current = matrix - dot3(left, split(jnp.concatenate(uppers, axis=1)))
        in_a, in_b = row_block == a, row_block == b
        mine = [
            lax.dynamic_slice_in_dim(m, own * block, block, 1) for m in (m_a, m_b)
        ]
        final = (
            jnp.where(in_a, ca[:, :block], mine[0]),
            jnp.where(in_a, cb[:, :block], jnp.where(in_b, new_b[:, :block], mine[1])),
        )
        for values, offset, is_owner in zip(final, offsets, owns):
            old = lax.dynamic_slice_in_dim(current, offset, block, 1)
            current = lax.dynamic_update_slice_in_dim(
                current, jnp.where(is_owner, values, old), offset, 1
            )
        factored = current.astype(BF16)
    totals = sums
    for k in range(row_count.bit_length() - 1):
        moved = lax.ppermute(totals, "row", [(i, i ^ 1 << k) for i in range(row_count)])
        totals = totals + moved
    if len(tokens) > 1:
        totals = totals + tokens[0][0, 0]
    rhs_norms = jnp.sqrt(totals / total_rows + 1e-06)
    return factored, new_rhs, rhs_norms


def solution(mesh):
    in_specs = (P("row", "col"), P("row", "col"), P(), P())
    out_specs = (P("row", "col"), P("row", "col"), P("col"))
    return jax.shard_map(
        on_device, mesh=mesh, in_specs=in_specs, out_specs=out_specs, check_vma=False
    )
```
